32 devices in a mesh: expert: 8 (over z, x), mp: 4 (over y, core).
Axes of the slice: x: 2, y: 2, z: 4, core: 2. Of those that a mesh axis runs over, the one named last changes fastest.
Arguments:
- base_weights: bfloat16 [8, 7168, 1024], P('expert', 'mp'), may hold values from -6 to 6
- deltas: bfloat16 [3, 8, 7168, 1024], P(None, 'expert', 'mp'), may hold values from -1.6 to 1.6
- keep_flags: int32 [3, 8, 896, 8], P(None, 'expert', 'mp'), may hold values 0 or 1
- serve_order: int32 [8], replicated, may hold values from 0 to 7, each once
Outputs:
- served_weights: bfloat16 [8, 1024, 7168], P(None, 'expert', 'mp')
- checksums: float32 [8], P('expert')
- largest_change: float32 [8], P('expert')
The draws below stay inside these ranges and needn't reach their ends.
Inputs may be any that keep to these rules, and one draw needn't show every extreme that they name: `serve_order`: each expert appears in exactly one slot.
All inputs are finite; a program needn't handle non-finite values. No bound on the sum of `keep_flags` on one device may be relied on, other than what follows from the above.
Results may differ from the reference program's by a relative error of at most 0.008.
Values may be sent and summed in bfloat16 or wider, within the bound.
A program may use at most 64 MiB of HBM per device.

```python
import math
import jax
import jax.numpy as jnp
from jax import lax

D = 7168
F = 1024
CKPTS = 3
EXPERTS = 8


def draw_deltas(key, part):
    folded = jax.random.fold_in(key, 11)
    key_scale, key_value = jax.random.split(folded)
    key_band = jax.random.fold_in(folded, 23)
    scales = jnp.exp(jax.random.uniform(key_scale, (1, EXPERTS, 1, 1, 1), jnp.float32, math.log(0.03), math.log(0.13)))
    bands = jnp.exp(jax.random.uniform(key_band, (1, EXPERTS, 8, 1, 1), jnp.float32, math.log(0.3), math.log(3.0)))
    values = jnp.clip(jax.random.normal(key_value, (CKPTS, EXPERTS, 8, D // 8, F), jnp.float32), -4.0, 4.0)
    shaped = (values * scales * bands).reshape(CKPTS, EXPERTS, D, F)
    return shaped.astype(jnp.bfloat16)


def set_ends(entries, own_key, smallest, high):
    longest = entries.shape.index(max(entries.shape))
    spots = []
    for shift in (0, 1):
        where = [jax.random.randint(jax.random.fold_in(own_key, axis), (), 0, length) for axis, length in enumerate(entries.shape)]
        where[longest] = (where[longest] + shift) % entries.shape[longest]
        spots.append(tuple(where))
    return entries.at[spots[0]].set(smallest).at[spots[1]].set(high)


def shard_levels(own_key, dims, shards, smallest, high):
    def one(axis_at, parts):
        draws = jax.random.uniform(jax.random.fold_in(jax.random.fold_in(own_key, 6), axis_at), (parts,), jnp.float32, smallest / len(shards), high / len(shards))
        return jnp.repeat(jnp.exp(draws), dims[axis_at] // parts).reshape((-1,) + (1,) * (len(dims) - axis_at - 1))

    loudness = one(*shards[0])
    for cut in shards[1:]:
        loudness = loudness * one(*cut)
    return loudness


def noise(stream_key, shape, spread, most, cuts=(), kind=jnp.bfloat16):
    factor_of = shard_levels(stream_key, shape, cuts, -0.22, 0.18) if cuts else 1.0
    drawn = jax.random.normal(stream_key, shape, jnp.float32) * spread * factor_of
    return jnp.minimum(jnp.maximum(drawn, -most), most).astype(kind)


def setup_inputs(seed: int = 0) -> dict:
    keys = jax.random.split(jax.random.key(seed), 5)
    base_weights = noise(keys[0], (EXPERTS, D, F), 1.0, 6.0, ((0, 8), (1, 4)))
    deltas = draw_deltas(jax.random.fold_in(keys[4], 71), 0)
    keep_flags = set_ends((jax.random.randint(keys[2], (CKPTS, EXPERTS, D // 8, F // 128), 0, 3) < 1).astype(jnp.int32), jax.random.fold_in(keys[2], 1), 0, 1)
    serve_order = jax.random.permutation(keys[3], EXPERTS).astype(jnp.int32)
    return dict(base_weights=base_weights, deltas=deltas, keep_flags=keep_flags, serve_order=serve_order)


def merge_block(base_rows, delta_rows, keep_rows):
    experts_here, row_count, columns = base_rows.shape
    expanded = keep_rows.astype(jnp.float32)[:, :, :, None, :, None]
    trimmed = delta_rows.astype(jnp.float32).reshape(3, experts_here, row_count // 8, 8, columns // 128, 128) * expanded
    trimmed = trimmed.reshape(3, experts_here, row_count, columns)
    elected = jnp.sign(trimmed[0] + trimmed[1] + trimmed[2])
    agreeing = (trimmed * elected > 0).astype(jnp.float32)
    voters = lax.optimization_barrier(jnp.sum(agreeing, axis=0))
    update = lax.optimization_barrier(jnp.sum(trimmed * agreeing, axis=0)) / jnp.maximum(voters, 1.0)
    merged = (base_rows.astype(jnp.float32) + update).astype(jnp.bfloat16)
    return (merged, update)

def reference(base_weights, deltas, keep_flags, serve_order):

    def per_expert(bundle):
        base_one, delta_one, keep_one = bundle
        merged, update = merge_block(base_one[None], delta_one[:, None], keep_one[:, None])
        checksum = jnp.sum(merged.astype(jnp.float32)) / math.sqrt(D * F)
        largest = jnp.max(jnp.abs(update))
        return (jnp.swapaxes(merged[0], 0, 1), checksum, largest)
    serving, checks, largest = lax.map(per_expert, (base_weights, jnp.moveaxis(deltas, 1, 0), jnp.moveaxis(keep_flags, 1, 0)))
    return (jnp.take(serving, serve_order, axis=0), checks, largest)
```

```python
import functools
import math

import jax
import jax.numpy as jnp
from jax import lax
from jax.experimental import pallas as pl
from jax.experimental.pallas import tpu as pltpu
from jax.sharding import PartitionSpec as P

MESH = pl.DeviceIdType.MESH
LANES = 128


def partner(me, mask, count):
    if count & (count - 1):
        return lax.rem(mask + count - me, count)
    out = 0
    bit = 1
    while bit < count:
        out = out + bit * lax.rem(me // bit + mask // bit, 2)
        bit *= 2
    return out


def exchange_kernel(
    n, m, scale, sub_rows, base_ref, delta_ref, keep_ref, out_ref, stat_ref,
    base_buf, delta_buf, keep_buf, flag_buf, send_buf, acc, stat_buf,
    base_sem, delta_sem, keep_sem, send_sem, recv_sem, stat_send_sem, stat_recv_sem,
):
    e = lax.axis_index("expert")
    p = lax.axis_index("mp")
    rows, columns = base_buf.shape[1], base_ref.shape[2]
    blocks = columns // LANES
    served = columns // n
    per_block = LANES // served
    subs = rows // sub_rows

    barrier = pltpu.get_barrier_semaphore()
    for k in range(1, n):
        pl.semaphore_signal(barrier, inc=1, device_id=(lax.rem(e + k, n), p), device_id_type=MESH)
    for k in range(1, m):
        pl.semaphore_signal(barrier, inc=1, device_id=(e, lax.rem(p + k, m)), device_id_type=MESH)

    def block_at(i):
        if blocks % 2:
            return partner(e // per_block, lax.rem(i + 1, blocks), blocks)
        half = blocks // 2
        late = i // half
        mask = (1 - late) * (half + i) + late * lax.rem(i + 1, half)
        return partner(e // per_block, mask, blocks)

    def loads(i, start=0, count=rows, sem=None):
        at = pl.ds(pl.multiple_of(block_at(i) * LANES, LANES), LANES)
        part = pl.ds(start, count)
        sem = i if sem is None else sem
        return (
            pltpu.make_async_copy(base_ref.at[0, part, at], base_buf.at[i, part], base_sem.at[sem]),
            pltpu.make_async_copy(delta_ref.at[:, 0, part, at], delta_buf.at[i, :, part], delta_sem.at[sem]),
        )

    head = loads(0, 0, sub_rows)
    rest = loads(0, sub_rows, rows - sub_rows, blocks)
    keep_load = pltpu.make_async_copy(keep_ref.at[:, 0], keep_buf, keep_sem)

    keep_load.start()
    for copy in head + rest:
        copy.start()
    acc[...] = jnp.zeros_like(acc)
    keep_load.wait()

    def send(i, j, target, lanes, source):
        return pltpu.make_async_remote_copy(
            src_ref=send_buf.at[i, pl.ds(j * served, served), lanes],
            dst_ref=out_ref.at[source, :, lanes],
            send_sem=send_sem.at[target],
            recv_sem=recv_sem.at[source],
            device_id=(target, p),
            device_id_type=MESH,
        )

    def merge(i, row):
        row = pl.multiple_of(row, LANES)
        trimmed = []
        for k in range(3):
            flags = flag_buf[k, pl.ds(pl.multiple_of(row // 8, LANES // 8), LANES // 8), :]
            flags = jnp.broadcast_to(flags[:, None, :], (LANES // 8, 8, LANES)).reshape(LANES, LANES)
            trimmed.append(delta_buf[i, k, pl.ds(row, LANES), :].astype(jnp.float32) * flags)
        total = (trimmed[0] + trimmed[1]) + trimmed[2]
        elected = jnp.where(total > 0, 1.0, jnp.where(total < 0, -1.0, 0.0))
        voters = jnp.zeros((LANES, LANES), jnp.float32)
        size = jnp.zeros((LANES, LANES), jnp.float32)
        for one in trimmed:
            toward = one * elected
            size = size + jnp.maximum(toward, 0.0)
            voters = voters + jnp.where(toward > 0, 1.0, 0.0)
        size = size * jnp.where(voters > 2.5, 1.0 / 3.0, jnp.where(voters > 1.5, 0.5, 1.0))
        base = base_buf[i, pl.ds(row, LANES), :].astype(jnp.float32)
        merged = (base + size * elected).astype(jnp.bfloat16).astype(jnp.float32)
        acc[0] += jnp.sum(merged.reshape(LANES // 8, 8, LANES), axis=0)
        acc[1] = jnp.maximum(acc[1], jnp.max(size.reshape(LANES // 8, 8, LANES), axis=0))
        send_buf[i, :, pl.ds(row, LANES)] = merged.T.astype(jnp.bfloat16)

    def block_step(i, carry):
        block = block_at(i)
        for k in range(3):
            here = keep_buf[k].astype(jnp.float32)
            pick = lax.broadcasted_iota(jnp.int32, (blocks, LANES), 0) == block
            flag_buf[k] = lax.dot_general(
                here, pick.astype(jnp.float32), (((0,), (0,)), ((), ())), preferred_element_type=jnp.float32
            )

        def sub_step(s, carry):
            @pl.when(i + s == 0)
            def _():
                for copy in head:
                    copy.wait()

            @pl.when(i * subs + s == 1)
            def _():
                for copy in rest:
                    copy.wait()

            @pl.when(i * subs - s * blocks * subs > 0)
            def _():
                for copy in loads(i):
                    copy.wait()

            @pl.when(i + 1 + s * blocks < blocks)
            def _():
                for copy in loads(i + 1):
                    copy.start()

            for r in range(sub_rows // LANES):
                merge(i, s * sub_rows + r * LANES)

            @pl.when(i + s == 0)
            def _():
                pl.semaphore_wait(barrier, n + m - 2)

            lanes = pl.ds(pl.multiple_of(s * sub_rows, LANES), sub_rows)
            for j in range(per_block):
                target = block * per_block + j

                @pl.when(target != e)
                def _():
                    send(i, j, target, lanes, e).start()

            return carry

        lax.fori_loop(0, subs, sub_step, 0)
        return carry

    lax.fori_loop(0, blocks, block_step, 0)

    stat_buf[p] = acc[...]

    def stat_copy(k):
        other = lax.rem(p + k, m)
        return other, pltpu.make_async_remote_copy(
            src_ref=acc,
            dst_ref=stat_buf.at[p],
            send_sem=stat_send_sem.at[other],
            recv_sem=stat_recv_sem.at[p],
            device_id=(e, other),
            device_id_type=MESH,
        )

    for k in range(1, m):
        stat_copy(k)[1].start()

    own = e - (e // per_block) * per_block
    for j in range(per_block):

        @pl.when(own == j)
        def _():
            out_ref[e] = send_buf[blocks - 1, pl.ds(j * served, served), :]

    for k in range(1, m):
        other, copy = stat_copy(k)
        copy.wait_send()
        pltpu.make_async_remote_copy(
            src_ref=acc,
            dst_ref=stat_buf.at[other],
            send_sem=stat_send_sem.at[other],
            recv_sem=stat_recv_sem.at[other],
            device_id=(e, other),
            device_id_type=MESH,
        ).wait_recv()
    value = stat_buf[0, 0]
    largest = stat_buf[0, 1]
    for k in range(1, m):
        value = value + stat_buf[k, 0]
        largest = jnp.maximum(largest, stat_buf[k, 1])
    stat_ref[0] = jnp.broadcast_to(jnp.sum(value, keepdims=True) / scale, (8, LANES))
    stat_ref[1] = jnp.broadcast_to(jnp.max(largest, keepdims=True), (8, LANES))

    everything = pl.ds(0, rows)

    def finish(k, carry):
        other = lax.rem(e + k, n)
        copy = send(0, 0, other, everything, other)
        copy.wait_send()
        copy.wait_recv()
        return carry

    lax.fori_loop(1, n, finish, 0)


def serve_kernel(order_ref, held_ref, stat_ref, out_ref, check_ref, largest_ref, check_buf, largest_buf, sems):
    slots = out_ref.shape[0]
    order = order_ref[...].astype(jnp.float32)
    copies = [
        pltpu.make_async_copy(
            held_ref.at[jnp.max(order[0:1, s : s + 1]).astype(jnp.int32)], out_ref.at[s], sems.at[s]
        )
        for s in range(slots)
    ]
    for copy in copies:
        copy.start()
    check_buf[0] = jnp.max(stat_ref[0, 0:1, 0:1])
    largest_buf[0] = jnp.max(stat_ref[1, 0:1, 0:1])
    small = [
        pltpu.make_async_copy(check_buf, check_ref, sems.at[slots]),
        pltpu.make_async_copy(largest_buf, largest_ref, sems.at[slots + 1]),
    ]
    for copy in small:
        copy.start()
    for copy in copies + small:
        copy.wait()


def in_hbm(x):
    return pltpu.with_memory_space_constraint(x, pltpu.HBM)


def on_device(n, m, base_weights, deltas, keep_flags, serve_order):
    _, rows, columns = base_weights.shape
    blocks = columns // LANES
    served = columns // n
    sub_rows = 2 * LANES if rows % (2 * LANES) == 0 else LANES
    hbm = pl.BlockSpec(memory_space=pltpu.HBM)
    vmem = pl.BlockSpec(memory_space=pltpu.VMEM)
    held, stats = pl.pallas_call(
        functools.partial(exchange_kernel, n, m, math.sqrt(rows * m * columns), sub_rows),
        out_shape=(
            jax.ShapeDtypeStruct((n, served, rows), jnp.bfloat16),
            jax.ShapeDtypeStruct((2, 8, LANES), jnp.float32),
        ),
        in_specs=[hbm] * 3,
        out_specs=(vmem, vmem),
        scratch_shapes=[
            pltpu.VMEM((blocks, rows, LANES), jnp.bfloat16),
            pltpu.VMEM((blocks, 3, rows, LANES), jnp.bfloat16),
            pltpu.VMEM((3, blocks, rows // 8), jnp.int32),
            pltpu.VMEM((3, rows // 8, LANES), jnp.float32),
            pltpu.VMEM((blocks, LANES, rows), jnp.bfloat16),
            pltpu.VMEM((2, 8, LANES), jnp.float32),
            pltpu.VMEM((m, 2, 8, LANES), jnp.float32),
            pltpu.SemaphoreType.DMA((blocks + 1,)),
            pltpu.SemaphoreType.DMA((blocks + 1,)),
            pltpu.SemaphoreType.DMA,
            pltpu.SemaphoreType.DMA((n,)),
            pltpu.SemaphoreType.DMA((n,)),
            pltpu.SemaphoreType.DMA((m,)),
            pltpu.SemaphoreType.DMA((m,)),
        ],
        compiler_params=pltpu.CompilerParams(
            collective_id=0, has_side_effects=True, vmem_limit_bytes=49 * 1024 * 1024
        ),
        name="exchange",
    )(in_hbm(base_weights), in_hbm(deltas), in_hbm(jnp.swapaxes(keep_flags, 2, 3)))
    return pl.pallas_call(
        serve_kernel,
        out_shape=(
            jax.ShapeDtypeStruct((n, served, rows), jnp.bfloat16),
            jax.ShapeDtypeStruct((1,), jnp.float32),
            jax.ShapeDtypeStruct((1,), jnp.float32),
        ),
        in_specs=[vmem, vmem, vmem],
        out_specs=(hbm, hbm, hbm),
        scratch_shapes=[
            pltpu.SMEM((1,), jnp.float32),
            pltpu.SMEM((1,), jnp.float32),
            pltpu.SemaphoreType.DMA((n + 2,)),
        ],
        compiler_params=pltpu.CompilerParams(vmem_limit_bytes=8 * 1024 * 1024),
        name="serve",
    )(serve_order.reshape(1, n), held, stats)


def solution(mesh):
    n, m = mesh.shape["expert"], mesh.shape["mp"]
    in_specs = (
        P("expert", "mp", None),
        P(None, "expert", "mp", None),
        P(None, "expert", "mp", None),
        P(),
    )
    out_specs = (P(None, "expert", "mp"), P("expert"), P("expert"))
    return jax.shard_map(
        functools.partial(on_device, n, m), mesh=mesh, in_specs=in_specs, out_specs=out_specs, check_vma=False
    )
```

```python
import functools
import math

import jax
import jax.numpy as jnp
from jax import lax
from jax.experimental import pallas as pl
from jax.experimental.pallas import tpu as pltpu
from jax.sharding import PartitionSpec as P

MESH = pl.DeviceIdType.MESH
LANES = 128


def partner(me, mask, count):
    if count & (count - 1):
        return lax.rem(mask + count - me, count)
    out = 0
    bit = 1
    while bit < count:
        out = out + bit * lax.rem(me // bit + mask // bit, 2)
        bit *= 2
    return out


def exchange_kernel(
    n, m, scale, sub_rows, base_ref, delta_ref, keep_ref, out_ref, stat_ref,
    base_buf, delta_buf, keep_buf, flag_buf, send_buf, acc, stat_buf,
    base_sem, delta_sem, keep_sem, send_sem, recv_sem, stat_send_sem, stat_recv_sem,
    known_sem,
):
    e = lax.axis_index("expert")
    p = lax.axis_index("mp")
    rows, columns = base_buf.shape[1], base_ref.shape[2]
    blocks = columns // LANES
    served = columns // n
    per_block = LANES // served
    subs = rows // sub_rows

    half, quarter = blocks // 2, blocks // 4
    mine = e // per_block
    lower = 1 - mine // half
    inner = lax.rem(mine // quarter + mine // half, 2)
    facing_inner = lower * half + (1 - lower) * quarter
    facing_outer = lower * (half + quarter)
    beside = partner(e, quarter * per_block, n)

    def block_at(i):
        stage = (i + quarter - 1) // quarter
        at_outer = stage * (2 - stage)
        far = at_outer * (facing_outer + i - 1) + (1 - at_outer) * facing_inner + stage // 2 * (i - quarter)
        near = partner(mine, lax.rem(i + 1, half), blocks)
        return (1 - i // half) * far + i // half * near

    def loads(i, start=0, count=rows, sem=None):
        at = pl.ds(pl.multiple_of(block_at(i) * LANES, LANES), LANES)
        part = pl.ds(start, count)
        sem = i if sem is None else sem
        return (
            pltpu.make_async_copy(base_ref.at[0, part, at], base_buf.at[i, part], base_sem.at[sem]),
            pltpu.make_async_copy(delta_ref.at[:, 0, part, at], delta_buf.at[i, :, part], delta_sem.at[sem]),
        )

    head = loads(0, 0, sub_rows)
    rest = loads(0, sub_rows, rows - sub_rows, blocks)
    keep_load = pltpu.make_async_copy(keep_ref.at[:, 0], keep_buf, keep_sem)

    keep_load.start()
    for copy in head + rest:
        copy.start()

    barrier = pltpu.get_barrier_semaphore()

    def greet(expert, place):
        pl.semaphore_signal(barrier, inc=1, device_id=(expert, place), device_id_type=MESH)

    @pl.when(inner - lax.rem(mine, quarter) == 1)
    def _():
        for k in range(quarter * per_block):
            greet(facing_inner * per_block + k, p)

    for k in range(1, n):
        other = lax.rem(e + k, n)
        block = other // per_block

        @pl.when(lax.rem(block // quarter + block // half, 2) == 0)
        def _():
            greet(other, p)

    for k in range(1, m):
        greet(inner * beside + (1 - inner) * e, lax.rem(p + k, m))
    acc[...] = jnp.zeros_like(acc)
    keep_load.wait()

    def send(i, j, target, lanes, source):
        return pltpu.make_async_remote_copy(
            src_ref=send_buf.at[i, pl.ds(j * served, served), lanes],
            dst_ref=out_ref.at[source, :, lanes],
            send_sem=send_sem.at[target],
            recv_sem=recv_sem.at[source],
            device_id=(target, p),
            device_id_type=MESH,
        )

    def merge(i, row):
        row = pl.multiple_of(row, LANES)
        trimmed = []
        for k in range(3):
            flags = flag_buf[k, pl.ds(pl.multiple_of(row // 8, LANES // 8), LANES // 8), :]
            flags = jnp.broadcast_to(flags[:, None, :], (LANES // 8, 8, LANES)).reshape(LANES, LANES)
            trimmed.append(delta_buf[i, k, pl.ds(row, LANES), :].astype(jnp.float32) * flags)
        total = (trimmed[0] + trimmed[1]) + trimmed[2]
        elected = jnp.where(total > 0, 1.0, jnp.where(total < 0, -1.0, 0.0))
        voters = jnp.zeros((LANES, LANES), jnp.float32)
        size = jnp.zeros((LANES, LANES), jnp.float32)
        for one in trimmed:
            toward = one * elected
            size = size + jnp.maximum(toward, 0.0)
            voters = voters + jnp.where(toward > 0, 1.0, 0.0)
        size = size * jnp.where(voters > 2.5, 1.0 / 3.0, jnp.where(voters > 1.5, 0.5, 1.0))
        base = base_buf[i, pl.ds(row, LANES), :].astype(jnp.float32)
        merged = (base + size * elected).astype(jnp.bfloat16).astype(jnp.float32)
        acc[0] += jnp.sum(merged.reshape(LANES // 8, 8, LANES), axis=0)
        acc[1] = jnp.maximum(acc[1], jnp.max(size.reshape(LANES // 8, 8, LANES), axis=0))
        send_buf[i, :, pl.ds(row, LANES)] = merged.T.astype(jnp.bfloat16)

    def block_step(i, carry):
        block = block_at(i)
        for k in range(3):
            here = keep_buf[k].astype(jnp.float32)
            pick = lax.broadcasted_iota(jnp.int32, (blocks, LANES), 0) == block
            flag_buf[k] = lax.dot_general(
                here, pick.astype(jnp.float32), (((0,), (0,)), ((), ())), preferred_element_type=jnp.float32
            )

        def sub_step(s, carry):
            @pl.when(i + s == 0)
            def _():
                for copy in head:
                    copy.wait()

            @pl.when(i * subs + s == 1)
            def _():
                for copy in rest:
                    copy.wait()

            @pl.when(i * subs - s * blocks * subs > 0)
            def _():
                for copy in loads(i):
                    copy.wait()

            @pl.when(i + 1 + s * blocks < blocks)
            def _():
                for copy in loads(i + 1):
                    copy.start()

            for r in range(sub_rows // LANES):
                merge(i, s * sub_rows + r * LANES)

            @pl.when(i + s + inner == 0)
            def _():
                pl.semaphore_wait(barrier, n - 1 + 2 * (m - 1))
                pl.semaphore_signal(known_sem, inc=1, device_id=(beside, p), device_id_type=MESH)

            @pl.when(i + s - inner == -1)
            def _():
                pl.semaphore_wait(barrier, per_block)

            @pl.when((i * subs + s) * inner == subs)
            def _():
                pl.semaphore_wait(known_sem, 1)

            lanes = pl.ds(pl.multiple_of(s * sub_rows, LANES), sub_rows)
            for j in range(per_block):
                target = block * per_block + j

                @pl.when(target != e)
                def _():
                    send(i, j, target, lanes, e).start()

            return carry

        lax.fori_loop(0, subs, sub_step, 0)
        return carry

    lax.fori_loop(0, blocks, block_step, 0)

    stat_buf[p] = acc[...]

    def stat_copy(k):
        other = lax.rem(p + k, m)
        return other, pltpu.make_async_remote_copy(
            src_ref=acc,
            dst_ref=stat_buf.at[p],
            send_sem=stat_send_sem.at[other],
            recv_sem=stat_recv_sem.at[p],
            device_id=(e, other),
            device_id_type=MESH,
        )

    for k in range(1, m):
        stat_copy(k)[1].start()

    own = e - (e // per_block) * per_block
    for j in range(per_block):

        @pl.when(own == j)
        def _():
            out_ref[e] = send_buf[blocks - 1, pl.ds(j * served, served), :]

    for k in range(1, m):
        other, copy = stat_copy(k)
        copy.wait_send()
        pltpu.make_async_remote_copy(
            src_ref=acc,
            dst_ref=stat_buf.at[other],
            send_sem=stat_send_sem.at[other],
            recv_sem=stat_recv_sem.at[other],
            device_id=(e, other),
            device_id_type=MESH,
        ).wait_recv()
    value = stat_buf[0, 0]
    largest = stat_buf[0, 1]
    for k in range(1, m):
        value = value + stat_buf[k, 0]
        largest = jnp.maximum(largest, stat_buf[k, 1])
    stat_ref[0] = jnp.broadcast_to(jnp.sum(value, keepdims=True) / scale, (8, LANES))
    stat_ref[1] = jnp.broadcast_to(jnp.max(largest, keepdims=True), (8, LANES))

    everything = pl.ds(0, rows)

    def finish(k, carry):
        other = lax.rem(e + k, n)
        copy = send(0, 0, other, everything, other)
        copy.wait_send()
        copy.wait_recv()
        return carry

    lax.fori_loop(1, n, finish, 0)


def serve_kernel(order_ref, held_ref, stat_ref, out_ref, check_ref, largest_ref, check_buf, largest_buf, sems):
    slots = out_ref.shape[0]
    order = order_ref[...].astype(jnp.float32)
    copies = [
        pltpu.make_async_copy(
            held_ref.at[jnp.max(order[0:1, s : s + 1]).astype(jnp.int32)], out_ref.at[s], sems.at[s]
        )
        for s in range(slots)
    ]
    for copy in copies:
        copy.start()
    check_buf[0] = jnp.max(stat_ref[0, 0:1, 0:1])
    largest_buf[0] = jnp.max(stat_ref[1, 0:1, 0:1])
    small = [
        pltpu.make_async_copy(check_buf, check_ref, sems.at[slots]),
        pltpu.make_async_copy(largest_buf, largest_ref, sems.at[slots + 1]),
    ]
    for copy in small:
        copy.start()
    for copy in copies + small:
        copy.wait()


def in_hbm(x):
    return pltpu.with_memory_space_constraint(x, pltpu.HBM)


def on_device(n, m, base_weights, deltas, keep_flags, serve_order):
    _, rows, columns = base_weights.shape
    blocks = columns // LANES
    served = columns // n
    sub_rows = 2 * LANES if rows % (2 * LANES) == 0 else LANES
    hbm = pl.BlockSpec(memory_space=pltpu.HBM)
    vmem = pl.BlockSpec(memory_space=pltpu.VMEM)
    held, stats = pl.pallas_call(
        functools.partial(exchange_kernel, n, m, math.sqrt(rows * m * columns), sub_rows),
        out_shape=(
            jax.ShapeDtypeStruct((n, served, rows), jnp.bfloat16),
            jax.ShapeDtypeStruct((2, 8, LANES), jnp.float32),
        ),
        in_specs=[hbm] * 3,
        out_specs=(vmem, vmem),
        scratch_shapes=[
            pltpu.VMEM((blocks, rows, LANES), jnp.bfloat16),
            pltpu.VMEM((blocks, 3, rows, LANES), jnp.bfloat16),
            pltpu.VMEM((3, blocks, rows // 8), jnp.int32),
            pltpu.VMEM((3, rows // 8, LANES), jnp.float32),
            pltpu.VMEM((blocks, LANES, rows), jnp.bfloat16),
            pltpu.VMEM((2, 8, LANES), jnp.float32),
            pltpu.VMEM((m, 2, 8, LANES), jnp.float32),
            pltpu.SemaphoreType.DMA((blocks + 1,)),
            pltpu.SemaphoreType.DMA((blocks + 1,)),
            pltpu.SemaphoreType.DMA,
            pltpu.SemaphoreType.DMA((n,)),
            pltpu.SemaphoreType.DMA((n,)),
            pltpu.SemaphoreType.DMA((m,)),
            pltpu.SemaphoreType.DMA((m,)),
            pltpu.SemaphoreType.REGULAR,
        ],
        compiler_params=pltpu.CompilerParams(
            collective_id=0, has_side_effects=True, vmem_limit_bytes=49 * 1024 * 1024
        ),
        name="exchange",
    )(in_hbm(base_weights), in_hbm(deltas), in_hbm(jnp.swapaxes(keep_flags, 2, 3)))
    return pl.pallas_call(
        serve_kernel,
        out_shape=(
            jax.ShapeDtypeStruct((n, served, rows), jnp.bfloat16),
            jax.ShapeDtypeStruct((1,), jnp.float32),
            jax.ShapeDtypeStruct((1,), jnp.float32),
        ),
        in_specs=[vmem, vmem, vmem],
        out_specs=(hbm, hbm, hbm),
        scratch_shapes=[
            pltpu.SMEM((1,), jnp.float32),
            pltpu.SMEM((1,), jnp.float32),
            pltpu.SemaphoreType.DMA((n + 2,)),
        ],
        compiler_params=pltpu.CompilerParams(vmem_limit_bytes=8 * 1024 * 1024),
        name="serve",
    )(serve_order.reshape(1, n), held, stats)


def solution(mesh):
    n, m = mesh.shape["expert"], mesh.shape["mp"]
    in_specs = (
        P("expert", "mp", None),
        P(None, "expert", "mp", None),
        P(None, "expert", "mp", None),
        P(),
    )
    out_specs = (P(None, "expert", "mp"), P("expert"), P("expert"))
    return jax.shard_map(
        functools.partial(on_device, n, m), mesh=mesh, in_specs=in_specs, out_specs=out_specs, check_vma=False
    )
```

```python
import functools
import math

import jax
import jax.numpy as jnp
from jax import lax
from jax.experimental import pallas as pl
from jax.experimental.pallas import tpu as pltpu
from jax.sharding import PartitionSpec as P

MESH = pl.DeviceIdType.MESH
LANES = 128


def partner(me, mask, count):
    if count & (count - 1):
        return lax.rem(mask + count - me, count)
    out = 0
    bit = 1
    while bit < count:
        out = out + bit * lax.rem(me // bit + mask // bit, 2)
        bit *= 2
    return out


def exchange_kernel(
    n, m, scale, sub_rows, base_ref, delta_ref, keep_ref, out_ref, stat_ref,
    base_buf, delta_buf, keep_buf, flag_buf, send_buf, acc, stat_buf,
    base_sem, delta_sem, keep_sem, send_sem, recv_sem, stat_send_sem, stat_recv_sem,
    known_sem,
):
    e = lax.axis_index("expert")
    p = lax.axis_index("mp")
    rows, columns = base_buf.shape[1], base_ref.shape[2]
    blocks = columns // LANES
    served = columns // n
    per_block = LANES // served
    subs = rows // sub_rows

    half, quarter = blocks // 2, blocks // 4
    mine = e // per_block
    lower = 1 - mine // half
    inner = lax.rem(mine // quarter + mine // half, 2)
    facing_inner = lower * half + (1 - lower) * quarter
    facing_outer = lower * (half + quarter)
    beside = partner(e, quarter * per_block, n)

    def block_at(i):
        stage = (i + quarter - 1) // quarter
        at_outer = stage * (2 - stage)
        far = at_outer * (facing_outer + i - 1) + (1 - at_outer) * facing_inner + stage // 2 * (i - quarter)
        near = partner(mine, lax.rem(i + 1, half), blocks)
        return (1 - i // half) * far + i // half * near

    def loads(i, start=0, count=rows, sem=None):
        at = pl.ds(pl.multiple_of(block_at(i) * LANES, LANES), LANES)
        part = pl.ds(start, count)
        sem = i if sem is None else sem
        return (
            pltpu.make_async_copy(base_ref.at[0, part, at], base_buf.at[i, part], base_sem.at[sem]),
            pltpu.make_async_copy(delta_ref.at[:, 0, part, at], delta_buf.at[i, :, part], delta_sem.at[sem]),
        )

    head = loads(0, 0, sub_rows)
    rest = loads(0, sub_rows, rows - sub_rows, blocks)
    keep_load = pltpu.make_async_copy(keep_ref.at[:, 0], keep_buf, keep_sem)

    keep_load.start()
    for copy in head + rest:
        copy.start()

    barrier = pltpu.get_barrier_semaphore()

    def greet(expert, place):
        pl.semaphore_signal(barrier, inc=1, device_id=(expert, place), device_id_type=MESH)

    @pl.when(inner - lax.rem(mine, quarter) == 1)
    def _():
        for k in range(quarter * per_block):
            greet(facing_inner * per_block + k, p)

    for k in range(1, n):
        other = lax.rem(e + k, n)
        block = other // per_block

        @pl.when(lax.rem(block // quarter + block // half, 2) == 0)
        def _():
            greet(other, p)

    for k in range(1, m):
        greet(inner * beside + (1 - inner) * e, lax.rem(p + k, m))
    acc[...] = jnp.zeros_like(acc)
    keep_load.wait()

    def send(i, j, target, lanes, source):
        return pltpu.make_async_remote_copy(
            src_ref=send_buf.at[i, pl.ds(j * served, served), lanes],
            dst_ref=out_ref.at[source, :, lanes],
            send_sem=send_sem.at[target],
            recv_sem=recv_sem.at[source],
            device_id=(target, p),
            device_id_type=MESH,
        )

    def merge(i, row):
        row = pl.multiple_of(row, LANES)
        trimmed = []
        for k in range(3):
            flags = flag_buf[k, pl.ds(pl.multiple_of(row // 8, LANES // 8), LANES // 8), :]
            flags = jnp.broadcast_to(flags[:, None, :], (LANES // 8, 8, LANES)).reshape(LANES, LANES)
            trimmed.append(delta_buf[i, k, pl.ds(row, LANES), :].astype(jnp.float32) * flags)
        total = (trimmed[0] + trimmed[1]) + trimmed[2]
        elected = jnp.where(total > 0, 1.0, jnp.where(total < 0, -1.0, 0.0))
        voters = jnp.zeros((LANES, LANES), jnp.float32)
        size = jnp.zeros((LANES, LANES), jnp.float32)
        for one in trimmed:
            toward = one * elected
            size = size + jnp.maximum(toward, 0.0)
            voters = voters + jnp.where(toward > 0, 1.0, 0.0)
        size = size * jnp.where(voters > 2.5, 1.0 / 3.0, jnp.where(voters > 1.5, 0.5, 1.0))
        base = base_buf[i, pl.ds(row, LANES), :].astype(jnp.float32)
        merged = (base + size * elected).astype(jnp.bfloat16).astype(jnp.float32)
        acc[0] += jnp.sum(merged.reshape(LANES // 8, 8, LANES), axis=0)
        acc[1] = jnp.maximum(acc[1], jnp.max(size.reshape(LANES // 8, 8, LANES), axis=0))
        send_buf[i, :, pl.ds(row, LANES)] = merged.T.astype(jnp.bfloat16)

    def block_step(i, carry):
        block = block_at(i)
        for k in range(3):
            here = keep_buf[k].astype(jnp.float32)
            pick = lax.broadcasted_iota(jnp.int32, (blocks, LANES), 0) == block
            flag_buf[k] = lax.dot_general(
                here, pick.astype(jnp.float32), (((0,), (0,)), ((), ())), preferred_element_type=jnp.float32
            )

        def sub_step(s, carry):
            @pl.when(i + s == 0)
            def _():
                for copy in head:
                    copy.wait()

            @pl.when(i * subs + s == 1)
            def _():
                for copy in rest:
                    copy.wait()

            @pl.when(i * subs - s * blocks * subs > 0)
            def _():
                for copy in loads(i):
                    copy.wait()

            @pl.when(i + 1 + s * blocks < blocks)
            def _():
                for copy in loads(i + 1):
                    copy.start()

            for r in range(sub_rows // LANES):
                merge(i, s * sub_rows + r * LANES)

            @pl.when(i + s + inner == 0)
            def _():
                pl.semaphore_wait(barrier, n - 1 + 2 * (m - 1))
                pl.semaphore_signal(known_sem, inc=1, device_id=(beside, p), device_id_type=MESH)

            @pl.when(i + s - inner == -1)
            def _():
                pl.semaphore_wait(barrier, per_block)

            @pl.when((i * subs + s) * inner == subs)
            def _():
                pl.semaphore_wait(known_sem, 1)

            lanes = pl.ds(pl.multiple_of(s * sub_rows, LANES), sub_rows)
            for j in range(per_block):
                target = block * per_block + j

                @pl.when(target != e)
                def _():
                    send(i, j, target, lanes, e).start()

            return carry

        lax.fori_loop(0, subs, sub_step, 0)
        return carry

    lax.fori_loop(0, blocks, block_step, 0)

    stat_buf[p] = acc[...]

    def stat_copy(k):
        other = lax.rem(p + k, m)
        return other, pltpu.make_async_remote_copy(
            src_ref=acc,
            dst_ref=stat_buf.at[p],
            send_sem=stat_send_sem.at[other],
            recv_sem=stat_recv_sem.at[p],
            device_id=(e, other),
            device_id_type=MESH,
        )

    for k in range(1, m):
        stat_copy(k)[1].start()

    own = e - (e // per_block) * per_block
    for j in range(per_block):

        @pl.when(own == j)
        def _():
            out_ref[e] = send_buf[blocks - 1, pl.ds(j * served, served), :]

    for k in range(1, m):
        other, copy = stat_copy(k)
        copy.wait_send()
        pltpu.make_async_remote_copy(
            src_ref=acc,
            dst_ref=stat_buf.at[other],
            send_sem=stat_send_sem.at[other],
            recv_sem=stat_recv_sem.at[other],
            device_id=(e, other),
            device_id_type=MESH,
        ).wait_recv()
    value = stat_buf[0, 0]
    largest = stat_buf[0, 1]
    for k in range(1, m):
        value = value + stat_buf[k, 0]
        largest = jnp.maximum(largest, stat_buf[k, 1])
    stat_ref[0] = jnp.broadcast_to(jnp.sum(value, keepdims=True) / scale, (8, LANES))
    stat_ref[1] = jnp.broadcast_to(jnp.max(largest, keepdims=True), (8, LANES))

    everything = pl.ds(0, rows)

    order = [*range(half, blocks), *range(1, quarter + 1), *range(quarter + 1, half), 0]
    for i in order:
        block = block_at(i)
        for j in range(per_block):
            other = block * per_block + j

            @pl.when(other != e)
            def _():
                send(0, 0, other, everything, other).wait_send()

    for i in order:
        block = block_at(i)
        for j in range(per_block):
            other = block * per_block + j

            @pl.when(other != e)
            def _():
                send(0, 0, other, everything, other).wait_recv()


def serve_kernel(order_ref, held_ref, stat_ref, out_ref, check_ref, largest_ref, check_buf, largest_buf, sems):
    slots = out_ref.shape[0]
    order = order_ref[...].astype(jnp.float32)
    copies = [
        pltpu.make_async_copy(
            held_ref.at[jnp.max(order[0:1, s : s + 1]).astype(jnp.int32)], out_ref.at[s], sems.at[s]
        )
        for s in range(slots)
    ]
    for copy in copies:
        copy.start()
    check_buf[0] = jnp.max(stat_ref[0, 0:1, 0:1])
    largest_buf[0] = jnp.max(stat_ref[1, 0:1, 0:1])
    small = [
        pltpu.make_async_copy(check_buf, check_ref, sems.at[slots]),
        pltpu.make_async_copy(largest_buf, largest_ref, sems.at[slots + 1]),
    ]
    for copy in small:
        copy.start()
    for copy in copies + small:
        copy.wait()


def in_hbm(x):
    return pltpu.with_memory_space_constraint(x, pltpu.HBM)


def on_device(n, m, base_weights, deltas, keep_flags, serve_order):
    _, rows, columns = base_weights.shape
    blocks = columns // LANES
    served = columns // n
    sub_rows = 2 * LANES if rows % (2 * LANES) == 0 else LANES
    hbm = pl.BlockSpec(memory_space=pltpu.HBM)
    vmem = pl.BlockSpec(memory_space=pltpu.VMEM)
    held, stats = pl.pallas_call(
        functools.partial(exchange_kernel, n, m, math.sqrt(rows * m * columns), sub_rows),
        out_shape=(
            jax.ShapeDtypeStruct((n, served, rows), jnp.bfloat16),
            jax.ShapeDtypeStruct((2, 8, LANES), jnp.float32),
        ),
        in_specs=[hbm] * 3,
        out_specs=(vmem, vmem),
        scratch_shapes=[
            pltpu.VMEM((blocks, rows, LANES), jnp.bfloat16),
            pltpu.VMEM((blocks, 3, rows, LANES), jnp.bfloat16),
            pltpu.VMEM((3, blocks, rows // 8), jnp.int32),
            pltpu.VMEM((3, rows // 8, LANES), jnp.float32),
            pltpu.VMEM((blocks, LANES, rows), jnp.bfloat16),
            pltpu.VMEM((2, 8, LANES), jnp.float32),
            pltpu.VMEM((m, 2, 8, LANES), jnp.float32),
            pltpu.SemaphoreType.DMA((blocks + 1,)),
            pltpu.SemaphoreType.DMA((blocks + 1,)),
            pltpu.SemaphoreType.DMA,
            pltpu.SemaphoreType.DMA((n,)),
            pltpu.SemaphoreType.DMA((n,)),
            pltpu.SemaphoreType.DMA((m,)),
            pltpu.SemaphoreType.DMA((m,)),
            pltpu.SemaphoreType.REGULAR,
        ],
        compiler_params=pltpu.CompilerParams(
            collective_id=0, has_side_effects=True, vmem_limit_bytes=49 * 1024 * 1024
        ),
        name="exchange",
    )(in_hbm(base_weights), in_hbm(deltas), in_hbm(jnp.swapaxes(keep_flags, 2, 3)))
    return pl.pallas_call(
        serve_kernel,
        out_shape=(
            jax.ShapeDtypeStruct((n, served, rows), jnp.bfloat16),
            jax.ShapeDtypeStruct((1,), jnp.float32),
            jax.ShapeDtypeStruct((1,), jnp.float32),
        ),
        in_specs=[vmem, vmem, vmem],
        out_specs=(hbm, hbm, hbm),
        scratch_shapes=[
            pltpu.SMEM((1,), jnp.float32),
            pltpu.SMEM((1,), jnp.float32),
            pltpu.SemaphoreType.DMA((n + 2,)),
        ],
        compiler_params=pltpu.CompilerParams(vmem_limit_bytes=8 * 1024 * 1024),
        name="serve",
    )(serve_order.reshape(1, n), held, stats)


def solution(mesh):
    n, m = mesh.shape["expert"], mesh.shape["mp"]
    in_specs = (
        P("expert", "mp", None),
        P(None, "expert", "mp", None),
        P(None, "expert", "mp", None),
        P(),
    )
    out_specs = (P(None, "expert", "mp"), P("expert"), P("expert"))
    return jax.shard_map(
        functools.partial(on_device, n, m), mesh=mesh, in_specs=in_specs, out_specs=out_specs, check_vma=False
    )
```

```python
import functools
import math

import jax
import jax.numpy as jnp
from jax import lax
from jax.experimental import pallas as pl
from jax.experimental.pallas import tpu as pltpu
from jax.sharding import PartitionSpec as P

MESH = pl.DeviceIdType.MESH
LANES = 128


def partner(me, mask, count):
    if count & (count - 1):
        return lax.rem(mask + count - me, count)
    out = 0
    bit = 1
    while bit < count:
        out = out + bit * lax.rem(me // bit + mask // bit, 2)
        bit *= 2
    return out


def exchange_kernel(
    n, m, scale, sub_rows, base_ref, delta_ref, keep_ref, out_ref, stat_ref,
    base_buf, delta_buf, keep_buf, flag_buf, send_buf, acc, stat_buf,
    base_sem, delta_sem, keep_sem, send_sem, recv_sem, stat_send_sem, stat_recv_sem,
    known_sem,
):
    e = lax.axis_index("expert")
    p = lax.axis_index("mp")
    rows, columns = base_buf.shape[1], base_ref.shape[2]
    blocks = columns // LANES
    served = columns // n
    per_block = LANES // served
    subs = rows // sub_rows

    half, quarter = blocks // 2, blocks // 4
    mine = e // per_block
    lower = 1 - mine // half
    inner = lax.rem(mine // quarter + mine // half, 2)
    facing_inner = lower * half + (1 - lower) * quarter
    facing_outer = lower * (half + quarter)
    beside = partner(e, quarter * per_block, n)

    def block_at(i):
        stage = (i + quarter - 1) // quarter
        at_outer = stage * (2 - stage)
        far = at_outer * (facing_outer + i - 1) + (1 - at_outer) * facing_inner + stage // 2 * (i - quarter)
        near = partner(mine, lax.rem(i + 1, half), blocks)
        return (1 - i // half) * far + i // half * near

    def loads(i, start=0, count=rows, sem=None):
        at = pl.ds(pl.multiple_of(block_at(i) * LANES, LANES), LANES)
        part = pl.ds(start, count)
        sem = i if sem is None else sem
        return (
            pltpu.make_async_copy(base_ref.at[0, part, at], base_buf.at[i, part], base_sem.at[sem]),
            pltpu.make_async_copy(delta_ref.at[:, 0, part, at], delta_buf.at[i, :, part], delta_sem.at[sem]),
        )

    head = loads(0, 0, sub_rows)
    rest = loads(0, sub_rows, rows - sub_rows, blocks)
    keep_load = pltpu.make_async_copy(keep_ref.at[:, 0], keep_buf, keep_sem)

    keep_load.start()
    for copy in head + rest:
        copy.start()

    barrier = pltpu.get_barrier_semaphore()

    def greet(expert, place):
        pl.semaphore_signal(barrier, inc=1, device_id=(expert, place), device_id_type=MESH)

    @pl.when(inner - lax.rem(mine, quarter) == 1)
    def _():
        for k in range(quarter * per_block):
            greet(facing_inner * per_block + k, p)

    for k in range(1, n):
        other = lax.rem(e + k, n)
        block = other // per_block

        @pl.when(lax.rem(block // quarter + block // half, 2) == 0)
        def _():
            greet(other, p)

    for k in range(1, m):
        greet(inner * beside + (1 - inner) * e, lax.rem(p + k, m))
    acc[...] = jnp.zeros_like(acc)
    keep_load.wait()

    def send(i, j, target, lanes, source):
        return pltpu.make_async_remote_copy(
            src_ref=send_buf.at[i, pl.ds(j * served, served), lanes],
            dst_ref=out_ref.at[source, :, lanes],
            send_sem=send_sem.at[target],
            recv_sem=recv_sem.at[source],
            device_id=(target, p),
            device_id_type=MESH,
        )

    def merge(i, row):
        row = pl.multiple_of(row, LANES)
        trimmed = []
        for k in range(3):
            flags = flag_buf[k, pl.ds(pl.multiple_of(row // 8, LANES // 8), LANES // 8), :]
            flags = jnp.broadcast_to(flags[:, None, :], (LANES // 8, 8, LANES)).reshape(LANES, LANES)
            trimmed.append(delta_buf[i, k, pl.ds(row, LANES), :].astype(jnp.float32) * flags)
        total = (trimmed[0] + trimmed[1]) + trimmed[2]
        elected = jnp.where(total > 0, 1.0, jnp.where(total < 0, -1.0, 0.0))
        voters = jnp.zeros((LANES, LANES), jnp.float32)
        size = jnp.zeros((LANES, LANES), jnp.float32)
        for one in trimmed:
            toward = one * elected
            size = size + jnp.maximum(toward, 0.0)
            voters = voters + jnp.where(toward > 0, 1.0, 0.0)
        size = size * jnp.where(voters > 2.5, 1.0 / 3.0, jnp.where(voters > 1.5, 0.5, 1.0))
        base = base_buf[i, pl.ds(row, LANES), :].astype(jnp.float32)
        merged = (base + size * elected).astype(jnp.bfloat16).astype(jnp.float32)
        acc[0] += jnp.sum(merged.reshape(LANES // 8, 8, LANES), axis=0)
        acc[1] = jnp.maximum(acc[1], jnp.max(size.reshape(LANES // 8, 8, LANES), axis=0))
        send_buf[i, :, pl.ds(row, LANES)] = merged.T.astype(jnp.bfloat16)

    def block_step(i, carry):
        block = block_at(i)
        for k in range(3):
            here = keep_buf[k].astype(jnp.float32)
            pick = lax.broadcasted_iota(jnp.int32, (blocks, LANES), 0) == block
            flag_buf[k] = lax.dot_general(
                here, pick.astype(jnp.float32), (((0,), (0,)), ((), ())), preferred_element_type=jnp.float32
            )

        def sub_step(s, carry):
            @pl.when(i + s == 0)
            def _():
                for copy in head:
                    copy.wait()

            @pl.when(i * subs + s == 1)
            def _():
                for copy in rest:
                    copy.wait()

            @pl.when(i * subs - s * blocks * subs > 0)
            def _():
                for copy in loads(i):
                    copy.wait()

            @pl.when(i + 1 + s * blocks < blocks)
            def _():
                for copy in loads(i + 1):
                    copy.start()

            for r in range(sub_rows // LANES):
                merge(i, s * sub_rows + r * LANES)

            @pl.when(i + s + inner == 0)
            def _():
                pl.semaphore_wait(barrier, n - 1 + 2 * (m - 1))
                pl.semaphore_signal(known_sem, inc=1, device_id=(beside, p), device_id_type=MESH)

            @pl.when(i + s - inner == -1)
            def _():
                pl.semaphore_wait(barrier, per_block)

            @pl.when((i * subs + s) * inner == subs)
            def _():
                pl.semaphore_wait(known_sem, 1)

            def send_rows(start, count):
                lanes = pl.ds(pl.multiple_of(start, LANES), count)
                for j in range(per_block):
                    target = block * per_block + j

                    @pl.when(target != e)
                    def _():
                        send(i, j, target, lanes, e).start()

            @pl.when(i == 0)
            def _():
                send_rows(s * sub_rows, sub_rows)

            @pl.when((i > 0) & (s == subs - 1))
            def _():
                send_rows(0, rows)

            return carry

        lax.fori_loop(0, subs, sub_step, 0)
        return carry

    lax.fori_loop(0, blocks, block_step, 0)

    stat_buf[p] = acc[...]

    def stat_copy(k):
        other = lax.rem(p + k, m)
        return other, pltpu.make_async_remote_copy(
            src_ref=acc,
            dst_ref=stat_buf.at[p],
            send_sem=stat_send_sem.at[other],
            recv_sem=stat_recv_sem.at[p],
            device_id=(e, other),
            device_id_type=MESH,
        )

    for k in range(1, m):
        stat_copy(k)[1].start()

    own = e - (e // per_block) * per_block
    for j in range(per_block):

        @pl.when(own == j)
        def _():
            out_ref[e] = send_buf[blocks - 1, pl.ds(j * served, served), :]

    for k in range(1, m):
        other, copy = stat_copy(k)
        copy.wait_send()
        pltpu.make_async_remote_copy(
            src_ref=acc,
            dst_ref=stat_buf.at[other],
            send_sem=stat_send_sem.at[other],
            recv_sem=stat_recv_sem.at[other],
            device_id=(e, other),
            device_id_type=MESH,
        ).wait_recv()
    value = stat_buf[0, 0]
    largest = stat_buf[0, 1]
    for k in range(1, m):
        value = value + stat_buf[k, 0]
        largest = jnp.maximum(largest, stat_buf[k, 1])
    stat_ref[0] = jnp.broadcast_to(jnp.sum(value, keepdims=True) / scale, (8, LANES))
    stat_ref[1] = jnp.broadcast_to(jnp.max(largest, keepdims=True), (8, LANES))

    everything = pl.ds(0, rows)

    order = [*range(half, blocks), *range(1, quarter + 1), *range(quarter + 1, half), 0]
    for i in order:
        block = block_at(i)
        for j in range(per_block):
            other = block * per_block + j

            @pl.when(other != e)
            def _():
                send(0, 0, other, everything, other).wait_send()

    for i in order:
        block = block_at(i)
        for j in range(per_block):
            other = block * per_block + j

            @pl.when(other != e)
            def _():
                send(0, 0, other, everything, other).wait_recv()


def serve_kernel(order_ref, held_ref, stat_ref, out_ref, check_ref, largest_ref, check_buf, largest_buf, sems):
    slots = out_ref.shape[0]
    order = order_ref[...].astype(jnp.float32)
    copies = [
        pltpu.make_async_copy(
            held_ref.at[jnp.max(order[0:1, s : s + 1]).astype(jnp.int32)], out_ref.at[s], sems.at[s]
        )
        for s in range(slots)
    ]
    for copy in copies:
        copy.start()
    check_buf[0] = jnp.max(stat_ref[0, 0:1, 0:1])
    largest_buf[0] = jnp.max(stat_ref[1, 0:1, 0:1])
    small = [
        pltpu.make_async_copy(check_buf, check_ref, sems.at[slots]),
        pltpu.make_async_copy(largest_buf, largest_ref, sems.at[slots + 1]),
    ]
    for copy in small:
        copy.start()
    for copy in copies + small:
        copy.wait()


def in_hbm(x):
    return pltpu.with_memory_space_constraint(x, pltpu.HBM)


def on_device(n, m, base_weights, deltas, keep_flags, serve_order):
    _, rows, columns = base_weights.shape
    blocks = columns // LANES
    served = columns // n
    sub_rows = 2 * LANES if rows % (2 * LANES) == 0 else LANES
    hbm = pl.BlockSpec(memory_space=pltpu.HBM)
    vmem = pl.BlockSpec(memory_space=pltpu.VMEM)
    held, stats = pl.pallas_call(
        functools.partial(exchange_kernel, n, m, math.sqrt(rows * m * columns), sub_rows),
        out_shape=(
            jax.ShapeDtypeStruct((n, served, rows), jnp.bfloat16),
            jax.ShapeDtypeStruct((2, 8, LANES), jnp.float32),
        ),
        in_specs=[hbm] * 3,
        out_specs=(vmem, vmem),
        scratch_shapes=[
            pltpu.VMEM((blocks, rows, LANES), jnp.bfloat16),
            pltpu.VMEM((blocks, 3, rows, LANES), jnp.bfloat16),
            pltpu.VMEM((3, blocks, rows // 8), jnp.int32),
            pltpu.VMEM((3, rows // 8, LANES), jnp.float32),
            pltpu.VMEM((blocks, LANES, rows), jnp.bfloat16),
            pltpu.VMEM((2, 8, LANES), jnp.float32),
            pltpu.VMEM((m, 2, 8, LANES), jnp.float32),
            pltpu.SemaphoreType.DMA((blocks + 1,)),
            pltpu.SemaphoreType.DMA((blocks + 1,)),
            pltpu.SemaphoreType.DMA,
            pltpu.SemaphoreType.DMA((n,)),
            pltpu.SemaphoreType.DMA((n,)),
            pltpu.SemaphoreType.DMA((m,)),
            pltpu.SemaphoreType.DMA((m,)),
            pltpu.SemaphoreType.REGULAR,
        ],
        compiler_params=pltpu.CompilerParams(
            collective_id=0, has_side_effects=True, vmem_limit_bytes=49 * 1024 * 1024
        ),
        name="exchange",
    )(in_hbm(base_weights), in_hbm(deltas), in_hbm(jnp.swapaxes(keep_flags, 2, 3)))
    return pl.pallas_call(
        serve_kernel,
        out_shape=(
            jax.ShapeDtypeStruct((n, served, rows), jnp.bfloat16),
            jax.ShapeDtypeStruct((1,), jnp.float32),
            jax.ShapeDtypeStruct((1,), jnp.float32),
        ),
        in_specs=[vmem, vmem, vmem],
        out_specs=(hbm, hbm, hbm),
        scratch_shapes=[
            pltpu.SMEM((1,), jnp.float32),
            pltpu.SMEM((1,), jnp.float32),
            pltpu.SemaphoreType.DMA((n + 2,)),
        ],
        compiler_params=pltpu.CompilerParams(vmem_limit_bytes=8 * 1024 * 1024),
        name="serve",
    )(serve_order.reshape(1, n), held, stats)


def solution(mesh):
    n, m = mesh.shape["expert"], mesh.shape["mp"]
    in_specs = (
        P("expert", "mp", None),
        P(None, "expert", "mp", None),
        P(None, "expert", "mp", None),
        P(),
    )
    out_specs = (P(None, "expert", "mp"), P("expert"), P("expert"))
    return jax.shard_map(
        functools.partial(on_device, n, m), mesh=mesh, in_specs=in_specs, out_specs=out_specs, check_vma=False
    )
```
